256 devices in a mesh: seg: 64 (over z, x, core), bin: 4 (over y).
Axes of the slice: x: 4, y: 4, z: 8, core: 2. Of those that a mesh axis runs over, the one named last changes fastest.
Arguments:
- magnet_real: bfloat16 [512, 8, 32768], P('seg', None, 'bin'), may hold values from -8 to 8
- magnet_imag: bfloat16 [512, 8, 32768], P('seg', None, 'bin'), may hold values from -8 to 8
- detector_real: bfloat16 [512, 2, 32768], P('seg', None, 'bin'), may hold values from -8 to 8
- detector_imag: bfloat16 [512, 2, 32768], P('seg', None, 'bin'), may hold values from -8 to 8
- valid: int32 [512], P('seg'), may hold values 0 or 1
- intersection: float32 [32768], P('bin'), may hold values from 0.1 to 1
Outputs:
- cleaned_real: float32 [512, 32768], P('seg', 'bin')
- cleaned_imag: float32 [512, 32768], P('seg', 'bin')
- estimate: float32 [512], P('seg')
The draws below stay inside these ranges and needn't reach their ends.
Inputs may be any that keep to these rules, and one draw needn't show every extreme that they name: `valid`: 1 keeps a segment in the spectral sums, 0 vetoes it.
All inputs are finite; a program needn't handle non-finite values. No bound on the sum of `valid` on one device may be relied on, other than what follows from the above.
Results may differ from the reference program's by a relative error of at most 0.0005.
Values sent between devices are 32-bit elements; how exact they have to be, the bound alone decides.
A program may use at most 64 MiB of HBM per device.

```python
import math
import jax
import jax.numpy as jnp
from jax import lax

CHANNELS = 8
DETECTORS = 2
BINS = 32768
SEGS = 512


def schumann_sources(key):
    base = jax.random.fold_in(key, 9173)
    first, second = jax.random.split(base, 2)
    shape = (SEGS, 3, BINS)
    spread = 0.70710677
    src_real = jax.random.normal(first, shape, jnp.float32) * spread
    src_imag = jax.random.normal(second, shape, jnp.float32) * spread
    return (src_real, src_imag)


def complex_mixing(key, salt, rows):
    base = jax.random.fold_in(key, salt)
    first, second = jax.random.split(base, 2)
    spread = 0.57735027
    mix_real = jax.random.normal(first, (rows, 3, BINS), jnp.float32) * spread
    mix_imag = jax.random.normal(second, (rows, 3, BINS), jnp.float32) * spread
    return (mix_real, mix_imag)


def mixed_part(key, salt, rows, noise_scale, component):
    src_real, src_imag = schumann_sources(key)
    mix_real, mix_imag = complex_mixing(key, salt, rows)
    total = jnp.zeros((SEGS, rows, BINS), jnp.float32)
    for source in range(3):
        field_real = src_real[:, None, source, :]
        field_imag = src_imag[:, None, source, :]
        coeff_real = mix_real[None, :, source, :]
        coeff_imag = mix_imag[None, :, source, :]
        if component == 1:
            total = total + coeff_real * field_imag + coeff_imag * field_real
        else:
            total = total + coeff_real * field_real - coeff_imag * field_imag
    noise_key = jax.random.fold_in(key, salt + 1 + component)
    noise = jax.random.normal(noise_key, (SEGS, rows, BINS), jnp.float32) * noise_scale
    return total + noise


def magnet_component(key, component):
    values = mixed_part(key, 101, CHANNELS, 0.6, component)
    return jnp.clip(values, -8.0, 8.0).astype(jnp.bfloat16)


def detector_component(key, component):
    values = mixed_part(key, 211, DETECTORS, 0.7, component)
    return jnp.clip(values, -8.0, 8.0).astype(jnp.bfloat16)


def draw_magnet_real(key, part):
    return magnet_component(key, 0)


def draw_magnet_imag(key, part):
    return magnet_component(key, 1)


def draw_detector_real(key, part):
    return detector_component(key, 0)


def draw_detector_imag(key, part):
    return detector_component(key, 1)


def touch_ends(values, key, smallest, largest):
    longest = values.shape.index(max(values.shape))
    spots = []
    for shift in (0, 1):
        where = [jax.random.randint(jax.random.fold_in(key, axis), (), 0, length) for axis, length in enumerate(values.shape)]
        where[longest] = (where[longest] + shift) % values.shape[longest]
        spots.append(tuple(where))
    return values.at[spots[0]].set(smallest).at[spots[1]].set(largest)


def shard_levels(own_key, dims, cuts, least, top_value):
    loudness, own = 1.0, jax.random.fold_in(own_key, 6)
    for dim, parts in cuts:
        heights = jnp.exp(jax.random.uniform(jax.random.fold_in(own, dim), (parts,), jnp.float32, least / len(cuts), top_value / len(cuts)))
        loudness = loudness * jnp.repeat(heights, dims[dim] // parts).reshape([-1 if axis == dim else 1 for axis in range(len(dims))])
    return loudness


def setup_inputs(seed: int = 0) -> dict:
    seeds = jax.random.split(jax.random.key(seed), 7)
    return {
        "magnet_real": draw_magnet_real(jax.random.fold_in(seeds[6], 71), 0),
        "magnet_imag": draw_magnet_imag(jax.random.fold_in(seeds[6], 71), 0),
        "detector_real": draw_detector_real(jax.random.fold_in(seeds[6], 71), 0),
        "detector_imag": draw_detector_imag(jax.random.fold_in(seeds[6], 71), 0),
        "valid": touch_ends((jax.random.randint(seeds[4], (SEGS,), 0, 4) < 3).astype(jnp.int32), jax.random.fold_in(seeds[4], 1), 0, 1),
        "intersection": jnp.clip(jnp.exp(math.log(1.0) - 2.3025851 * jax.random.uniform(seeds[5], (BINS,), jnp.float32) ** shard_levels(seeds[5], (BINS,), ((0, 4),), -0.2, 0.2)), 0.1, 1.0),
    }


def wiener_solve(s_real, s_imag, p_real, p_imag):
    channels = s_real.shape[0]
    matrix_size = 2 * channels

    def matrix_entry(i, j):
        if i < channels and j < channels:
            value = s_real[i, j]
        elif i < channels:
            value = -s_imag[i, j - channels]
        elif j < channels:
            value = s_imag[i - channels, j]
        else:
            value = s_real[i - channels, j - channels]
        if i == j:
            value = value + 1.0
        return value

    def right_entry(i):
        if i < channels:
            return p_real[i]
        return p_imag[i - channels]
    factor = [[None] * matrix_size for i in range(matrix_size)]
    for j in range(matrix_size):
        running = matrix_entry(j, j)
        for k in range(j):
            running = running - factor[j][k] * factor[j][k]
        factor[j][j] = jnp.sqrt(running)
        inverse = 1.0 / factor[j][j]
        for i in range(j + 1, matrix_size):
            running = matrix_entry(i, j)
            for k in range(j):
                running = running - factor[i][k] * factor[j][k]
            factor[i][j] = running * inverse
    forward = []
    for i in range(matrix_size):
        running = right_entry(i)
        for k in range(i):
            running = running - factor[i][k] * forward[k]
        forward.append(running / factor[i][i])
    backward = [None] * matrix_size
    for i in reversed(range(matrix_size)):
        running = forward[i]
        for k in range(i + 1, matrix_size):
            running = running - factor[k][i] * backward[k]
        backward[i] = running / factor[i][i]
    return (jnp.stack(backward[:channels]), jnp.stack(backward[channels:]))

def reference(magnet_real, magnet_imag, detector_real, detector_imag, valid, intersection):
    block_bins = math.gcd(BINS, 1024)
    block_count = BINS // block_bins
    keep = valid.astype(jnp.float32)[:, None, None]

    def contract(left, right):
        return jnp.einsum('scf,sdf->cdf', left, right, precision=lax.Precision.HIGHEST)

    def project(filt, field):
        return jnp.einsum('ckf,scf->skf', filt, field, precision=lax.Precision.HIGHEST)

    def block_work(start):
        field_real = lax.dynamic_slice_in_dim(magnet_real, start, block_bins, 2).astype(jnp.float32)
        field_imag = lax.dynamic_slice_in_dim(magnet_imag, start, block_bins, 2).astype(jnp.float32)
        strain_real = lax.dynamic_slice_in_dim(detector_real, start, block_bins, 2).astype(jnp.float32)
        strain_imag = lax.dynamic_slice_in_dim(detector_imag, start, block_bins, 2).astype(jnp.float32)
        kept_real = field_real * keep
        kept_imag = field_imag * keep
        s_real = contract(kept_real, field_real) + contract(kept_imag, field_imag)
        s_imag = contract(kept_imag, field_real) - contract(kept_real, field_imag)
        p_real = contract(kept_real, strain_real) + contract(kept_imag, strain_imag)
        p_imag = contract(kept_imag, strain_real) - contract(kept_real, strain_imag)
        filt_real, filt_imag = wiener_solve(s_real, s_imag, p_real, p_imag)
        clean_real = strain_real - project(filt_real, field_real) - project(filt_imag, field_imag)
        clean_imag = strain_imag - project(filt_real, field_imag) + project(filt_imag, field_real)
        cross_real = clean_real[:, 0] * clean_real[:, 1] + clean_imag[:, 0] * clean_imag[:, 1]
        cross_imag = clean_imag[:, 0] * clean_real[:, 1] - clean_real[:, 0] * clean_imag[:, 1]
        return (cross_real, cross_imag)
    block_starts = jnp.arange(block_count, dtype=jnp.int32) * block_bins
    real_blocks, imag_blocks = lax.map(block_work, block_starts)
    cleaned_real = jnp.moveaxis(real_blocks, 0, 1).reshape(SEGS, BINS)
    cleaned_imag = jnp.moveaxis(imag_blocks, 0, 1).reshape(SEGS, BINS)
    summed = jnp.dot(cleaned_real, intersection, precision=lax.Precision.HIGHEST)
    estimate = summed / jnp.sqrt(jnp.sum(intersection * intersection))
    return (cleaned_real, cleaned_imag, estimate)
```

```python
import jax
import jax.numpy as jnp
from jax import lax
from jax.experimental import pallas as pl
from jax.experimental.pallas import tpu as pltpu
from jax.sharding import Mesh
from jax.sharding import PartitionSpec as P

SEG = ("seg_0", "seg_1", "seg_2")
MESH = pl.DeviceIdType.MESH
F32 = jnp.float32
NZ, NX, NY = 8, 4, 4
LANES = 128
SEGS = 8
ROWS = 96
WROWS = 32
TILES = 64

ORDER0 = ((2, 0), (2, 1), (1, 1), (3, 0), (1, 0), (3, 1), (0, 0), (0, 1))
ORDER1 = (4, 3, 5, 2, 6, 1, 7, 0)


def row_ids():
    return lax.broadcasted_iota(jnp.int32, (8, LANES), 0)


def spread(a, j):
    return jnp.broadcast_to(a[j : j + 1, :], (8, LANES))


def spectra_tile(tile, mr, mi, dr, di, keep, hbuf, put):
    lanes = pl.ds(pl.multiple_of(tile * LANES, LANES), LANES)
    rows = row_ids()
    total = [jnp.zeros((8, LANES), F32) for _ in range(13)]
    held = [jnp.zeros((8, LANES), F32) for _ in range(4)]
    for s in range(SEGS):
        a = mr[s, :, lanes].astype(F32)
        b = mi[s, :, lanes].astype(F32)
        hr = dr[s, :, lanes].astype(F32)
        hi = di[s, :, lanes].astype(F32)
        v = keep[s]
        ka, kb = a * v, b * v
        total[0] += ka * a + kb * b
        for r in range(1, 5):
            ra, rb = pltpu.roll(a, 8 - r, 0), pltpu.roll(b, 8 - r, 0)
            total[2 * r - 1] += ka * ra + kb * rb
            total[2 * r] += kb * ra - ka * rb
        for k in range(2):
            pr, pi = spread(hr, k), spread(hi, k)
            total[9 + 2 * k] += ka * pr + kb * pi
            total[10 + 2 * k] += kb * pr - ka * pi
            held[2 * k] = jnp.where(rows == s, pr, held[2 * k])
            held[2 * k + 1] = jnp.where(rows == s, pi, held[2 * k + 1])
    total[7] = jnp.where(rows < 4, total[7], total[8])
    del total[8]
    for q in range(12):
        put(q, total[q])
    for q in range(4):
        hbuf[tile, 8 * q : 8 * q + 8, :] = held[q]


def solve(spec):
    rows = row_ids()
    re, im = [None] * 8, [None] * 8
    re[0], im[0] = spec[0], jnp.zeros((8, LANES), F32)
    for r in (1, 2, 3):
        re[r], im[r] = spec[2 * r - 1], spec[2 * r]
        re[8 - r] = pltpu.roll(re[r], r, 0)
        im[8 - r] = -pltpu.roll(im[r], r, 0)
    turned = pltpu.roll(spec[7], 4, 0)
    re[4] = jnp.where(rows < 4, spec[7], turned)
    im[4] = jnp.where(rows < 4, -turned, spec[7])
    cr, ci = [], []
    for d in range(8):
        a, b = re[d], im[d]
        for c in range(1, 8):
            a = jnp.where(rows == c, re[(d - c) % 8], a)
            b = jnp.where(rows == c, im[(d - c) % 8], b)
        cr.append(jnp.where(rows == d, a + 1.0, a))
        ci.append(b)
    cr += [spec[8], spec[10]]
    ci += [spec[9], spec[11]]
    inverse = []
    for j in range(8):
        inverse.append(1.0 / spread(cr[j], j))
        fr = jnp.where(rows > j, cr[j] * inverse[j], 0.0)
        fi = jnp.where(rows > j, ci[j] * inverse[j], 0.0)
        for d in range(j + 1, 10):
            pr, pi = spread(cr[d], j), spread(ci[d], j)
            cr[d] = cr[d] - (fr * pr - fi * pi)
            ci[d] = ci[d] - (fr * pi + fi * pr)
    out = []
    for k in (8, 9):
        yr, yi = cr[k], ci[k]
        wr, wi = jnp.zeros((8, LANES), F32), jnp.zeros((8, LANES), F32)
        for d in reversed(range(8)):
            xr, xi = spread(yr, d) * inverse[d], spread(yi, d) * inverse[d]
            wr = jnp.where(rows == d, xr, wr)
            wi = jnp.where(rows == d, xi, wi)
            yr = yr - (cr[d] * xr - ci[d] * xi)
            yi = yi - (cr[d] * xi + ci[d] * xr)
        out += [wr, wi]
    return out


def row_sums(parts):
    rows = row_ids()
    low = rows < 4
    merged = []
    for s in range(4):
        a, b = parts[s], parts[s + 4]
        merged.append(jnp.where(low, a, b) + pltpu.roll(jnp.where(low, b, a), 4, 0))
    for step in (2, 1):
        first = (rows & step) == 0
        merged = [
            jnp.where(
                first,
                merged[s] + pltpu.roll(merged[s], 8 - step, 0),
                merged[s + step] + pltpu.roll(merged[s + step], step, 0),
            )
            for s in range(step)
        ]
    return merged[0]


def clean_tile(tile, mr, mi, inter, wbuf, hbuf, out_r, out_i):
    lanes = pl.ds(pl.multiple_of(tile * LANES, LANES), LANES)
    w = [wbuf[tile, 8 * q : 8 * q + 8, :] for q in range(4)]
    parts = [[], [], [], []]
    for s in range(SEGS):
        a = mr[s, :, lanes].astype(F32)
        b = mi[s, :, lanes].astype(F32)
        for k in range(2):
            parts[2 * k].append(w[2 * k] * a + w[2 * k + 1] * b)
            parts[2 * k + 1].append(w[2 * k] * b - w[2 * k + 1] * a)
    g = [hbuf[tile, 8 * q : 8 * q + 8, :] - row_sums(parts[q]) for q in range(4)]
    real = g[0] * g[2] + g[1] * g[3]
    out_r[:, lanes] = real
    out_i[:, lanes] = g[1] * g[2] - g[0] * g[3]
    return real * inter[pl.ds(tile, 1), :]


def kernel(
    mr, mi, dr, di, keep, inter, out_r, out_i, est,
    acc, outbox, inbox, rbuf, pbuf, wbuf, hbuf, num, ybuf,
    p_send, p_recv, r_send, r_recv, q_send, q_recv, z_send, z_recv,
    x_send, x_recv, f_send, f_recv, w_send, w_recv, y_send, y_recv,
):
    z, x, c = lax.axis_index("seg_0"), lax.axis_index("seg_1"), lax.axis_index("seg_2")
    y = lax.axis_index("bin")

    def at_z(d):
        return {"seg_0": lax.rem(z + d, NZ)}

    def at_x(d):
        return {"seg_1": lax.rem(x + d, NX)}

    def at_y(d):
        return {"bin": lax.rem(y + d, NY)}

    partner = {"seg_2": 1 - c}

    barrier = pltpu.get_barrier_semaphore()
    peers = [at_z(d) for d in range(1, NZ)] + [at_x(d) for d in range(1, NX)]
    peers += [at_y(d) for d in range(1, NY)] + [partner]
    for peer in peers:
        pl.semaphore_signal(barrier, inc=1, device_id=peer, device_id_type=MESH)

    def copy(src, dst, send, recv, where):
        return pltpu.make_async_remote_copy(
            src_ref=src, dst_ref=dst, send_sem=send, recv_sem=recv,
            device_id=where, device_id_type=MESH,
        )

    def add_into(dst, at, src, first, count):
        def body(i, carry):
            for q in range(12):
                block = pl.ds(8 * q, 8)
                dst[at + i, block, :] = dst[at + i, block, :] + src[first + i, block, :]
            return carry

        lax.fori_loop(0, count, body, 0)

    on_core0 = c == 0

    def first_tiles(g):
        d, half = ORDER0[g]
        zero = lax.rem(x + d, NX) * 8 + 4 * half
        one = 32 + lax.rem(z + ORDER1[g], NZ) * 4
        return jnp.where(on_core0, zero, one), jnp.where(on_core0, one, zero)

    def make_group(g, tile, dst):
        def body(i, carry):
            def put(q, value):
                dst[4 * g + i, 8 * q : 8 * q + 8, :] = value

            spectra_tile(tile + i, mr, mi, dr, di, keep, hbuf, put)
            return carry

        lax.fori_loop(0, 4, body, 0)

    to_partner = [
        copy(outbox.at[pl.ds(4 * g, 4)], inbox.at[pl.ds(4 * g, 4)],
             p_send.at[g], p_recv.at[g], partner)
        for g in range(8)
    ]

    def hop(first, count, place, slot, way):
        where = {0: (at_x(1), at_x(3)), 1: (at_z(1), at_z(7))}[way // 2][way % 2]
        return copy(acc.at[pl.ds(first, count)], rbuf.at[pl.ds(place, count)],
                    r_send.at[slot], r_recv.at[slot], where)

    zero_hops = [
        [hop(0, 4, 0, 0, 0), hop(8, 4, 4, 1, 0), hop(16, 4, 8, 2, 0)],
        [hop(4, 4, 12, 3, 1), hop(12, 4, 16, 4, 1), hop(20, 4, 20, 5, 1)],
    ]
    up = [0, 6, 4, 14, 12, 22, 20]
    down = [2, 8, 10, 16, 18, 24, 26]
    one_hops = [
        [hop(up[m], 2, 2 * m, m, 2) for m in range(7)],
        [hop(down[m], 2, 14 + 2 * m, 7 + m, 3) for m in range(7)],
    ]

    def combine(g):
        to_partner[g].wait_recv()
        add_into(acc, 4 * g, inbox, 4 * g, 4)
        if g < 4:

            @pl.when(on_core0)
            def _():
                zero_hops[g % 2][g // 2].start()

        @pl.when(jnp.logical_not(on_core0))
        def _():
            if g == 0:
                one_hops[0][0].start()
                one_hops[1][0].start()
            if g == 1:
                one_hops[0][1].start()
            if g == 2:
                one_hops[1][1].start()

    for g in range(8):
        own, other = first_tiles(g)
        make_group(g, other, outbox)
        if g == 0:
            pl.semaphore_wait(barrier, len(peers))
        to_partner[g].start()
        make_group(g, own, acc)
        if g:
            combine(g - 1)
    combine(7)

    spec_at = jnp.where(on_core0, 24 + z, 28 + x)
    far_first = (4, 3, 5, 2, 6, 1, 7)
    zero_last = {
        d: copy(acc.at[24 + lax.rem(z + d, NZ)], pbuf.at[d], q_send.at[d], q_recv.at[d], at_z(d))
        for d in far_first
    }
    one_last = {
        d: copy(acc.at[28 + lax.rem(x + d, NX)], pbuf.at[d], q_send.at[d], q_recv.at[d], at_x(d))
        for d in (2, 1, 3)
    }

    @pl.when(on_core0)
    def _():
        for way in range(2):
            first, _, last = zero_hops[way]
            first.wait_recv()
            add_into(acc, 16 + 4 * way, rbuf, 12 * way, 4)
            last.start()
        for way in range(2):
            zero_hops[way][1].wait_recv()
            add_into(acc, 28 - 4 * way, rbuf, 4 + 12 * way, 4)
        for way in range(2):
            zero_hops[way][2].wait_recv()
            add_into(acc, 24 + 4 * way, rbuf, 8 + 12 * way, 4)
        for d in far_first:
            zero_last[d].start()
        for d in reversed(far_first):
            zero_last[d].wait_recv()
            add_into(acc, spec_at, pbuf, d, 1)

    @pl.when(jnp.logical_not(on_core0))
    def _():
        for m in range(7):
            for way in range(2):
                chunks = (up, down)[way]
                target = chunks[2] if m == 0 else (chunks[m + 2] if m < 5 else None)
                if target is None:
                    target = ((30, 28), (28, 30))[way][m - 5]
                one_hops[way][m].wait_recv()
                add_into(acc, target, rbuf, 14 * way + 2 * m, 2)
                if m < 5:
                    one_hops[way][m + 2].start()
        for d in (2, 1, 3):
            one_last[d].start()
        for d in (1, 3, 2):
            one_last[d].wait_recv()
            add_into(acc, spec_at, pbuf, d, 1)

    spec = [acc[spec_at, 8 * q : 8 * q + 8, :] for q in range(12)]
    filters = solve(spec)

    def tile_of(core, zz, xx):
        return jnp.where(core == 0, xx * 8 + zz, 32 + zz * 4 + xx)

    mine = tile_of(c, z, x)
    for q in range(4):
        wbuf[mine, 8 * q : 8 * q + 8, :] = filters[q]

    def w_copy(tile, send, recv, where):
        return copy(wbuf.at[tile], wbuf.at[tile], send, recv, where)

    along_z = {d: w_copy(mine, z_send.at[d], z_recv.at[d], at_z(d)) for d in far_first}
    for d in far_first:
        along_z[d].start()

    square = inter[0:8, :] * inter[0:8, :]
    for i in range(1, 8):
        square = square + inter[8 * i : 8 * i + 8, :] * inter[8 * i : 8 * i + 8, :]
    num[...] = jnp.zeros_like(num)

    def z_of(d):
        return lax.rem(z + NZ - d, NZ)

    def x_of(d):
        return lax.rem(x + NX - d, NX)

    def tile_from(core, dz, dx):
        return tile_of(core, z_of(dz), x_of(dx))

    def got(tile, sem, where):
        w_copy(tile, z_send.at[0], sem, where).wait_recv()

    def cleaned(tile):
        num[...] += clean_tile(tile, mr, mi, inter, wbuf, hbuf, out_r, out_i)

    near_first = (0, 1, 7, 2, 6, 3, 5, 4)
    sent = []

    def share(kind, d, tile):
        to_core = w_copy(tile, w_send.at[kind, d], w_recv.at[kind, d], partner)
        to_core.start()
        sent.append(to_core)

    for d in near_first:
        tile = tile_from(c, d, 0)
        if d:
            got(tile, z_recv.at[d], at_z(NZ - d))
        for way, dx in ((0, 1), (1, 3)):
            onward = w_copy(tile, x_send.at[way, d], x_recv.at[way, d], at_x(dx))
            onward.start()
            sent.append(onward)
        share(0, d, tile)
        cleaned(tile)
    for d in near_first:
        for way, dx in ((0, 1), (1, 3)):
            tile = tile_from(c, d, dx)
            got(tile, x_recv.at[way, d], at_x(NX - dx))
            if way == (near_first.index(d) % 2):
                onward = w_copy(tile, f_send.at[d], f_recv.at[d], at_x(dx))
                onward.start()
                sent.append(onward)
            share(dx, d, tile)
            cleaned(tile)
    for d in near_first:
        tile = tile_from(c, d, 2)
        got(tile, f_recv.at[d], at_x(1 if near_first.index(d) % 2 == 1 else 3))
        share(2, d, tile)
    for dx in (0, 1, 3):
        for d in near_first:
            tile = tile_from(1 - c, d, dx)
            got(tile, w_recv.at[dx, d], partner)
            cleaned(tile)
    for d in near_first:
        cleaned(tile_from(c, d, 2))
    for d in near_first:
        tile = tile_from(1 - c, d, 2)
        got(tile, w_recv.at[2, d], partner)
        cleaned(tile)

    ybuf[y, 0:8, :] = num[...]
    ybuf[y, 8:16, :] = square
    over_y = [
        copy(ybuf.at[y], ybuf.at[y], y_send.at[d], y_recv.at[d], at_y(d)) for d in range(1, NY)
    ]
    for step in over_y:
        step.start()
    for d in range(1, NY):
        src = lax.rem(y + NY - d, NY)
        copy(ybuf.at[src], ybuf.at[src], y_send.at[d], y_recv.at[d], at_y(NY - d)).wait_recv()
    top, norm = ybuf[0, 0:8, :], ybuf[0, 8:16, :]
    for i in range(1, NY):
        top, norm = top + ybuf[i, 0:8, :], norm + ybuf[i, 8:16, :]
    top = jnp.sum(top, axis=1, keepdims=True)
    norm = jnp.sum(jnp.sum(norm, axis=1, keepdims=True), axis=0, keepdims=True)
    value = jnp.broadcast_to(top / jnp.sqrt(norm), (8, LANES))
    diagonal = row_ids() == lax.broadcasted_iota(jnp.int32, (8, LANES), 1)
    est[...] = jnp.sum(jnp.where(diagonal, value, 0.0), axis=0, keepdims=True)

    for step in over_y + sent + [along_z[d] for d in far_first] + to_partner:
        step.wait_send()

    @pl.when(on_core0)
    def _():
        for step in zero_hops[0] + zero_hops[1] + [zero_last[d] for d in far_first]:
            step.wait_send()

    @pl.when(jnp.logical_not(on_core0))
    def _():
        for step in one_hops[0] + one_hops[1] + [one_last[d] for d in (2, 1, 3)]:
            step.wait_send()


def on_device(magnet_real, magnet_imag, detector_real, detector_imag, valid, intersection):
    bins = magnet_real.shape[2]
    assert bins == TILES * LANES and magnet_real.shape[:2] == (SEGS, 8)
    dma = pltpu.SemaphoreType.DMA
    vmem = pl.BlockSpec(memory_space=pltpu.VMEM)
    smem = pl.BlockSpec(memory_space=pltpu.SMEM)
    cleaned_real, cleaned_imag, estimate = pl.pallas_call(
        kernel,
        out_shape=(
            jax.ShapeDtypeStruct((SEGS, bins), F32),
            jax.ShapeDtypeStruct((SEGS, bins), F32),
            jax.ShapeDtypeStruct((1, LANES), F32),
        ),
        in_specs=[vmem, vmem, vmem, vmem, smem, vmem],
        out_specs=(vmem, vmem, vmem),
        scratch_shapes=[
            pltpu.VMEM((32, ROWS, LANES), F32),
            pltpu.VMEM((32, ROWS, LANES), F32),
            pltpu.VMEM((32, ROWS, LANES), F32),
            pltpu.VMEM((28, ROWS, LANES), F32),
            pltpu.VMEM((8, ROWS, LANES), F32),
            pltpu.VMEM((TILES, WROWS, LANES), F32),
            pltpu.VMEM((TILES, 32, LANES), F32),
            pltpu.VMEM((8, LANES), F32),
            pltpu.VMEM((NY, 16, LANES), F32),
            dma((8,)), dma((8,)), dma((14,)), dma((14,)), dma((8,)), dma((8,)),
            dma((8,)), dma((8,)), dma((2, 8)), dma((2, 8)), dma((8,)), dma((8,)),
            dma((4, 8)), dma((4, 8)), dma((4,)), dma((4,)),
        ],
        compiler_params=pltpu.CompilerParams(collective_id=0, has_side_effects=True),
    )(
        magnet_real, magnet_imag, detector_real, detector_imag,
        valid.astype(F32), intersection.reshape(TILES, LANES),
    )
    return cleaned_real, cleaned_imag, estimate[0, :SEGS]


def solution(mesh):
    assert mesh.shape["seg"] == NZ * NX * 2 and mesh.shape["bin"] == NY
    torus = Mesh(mesh.devices.reshape(NZ, NX, 2, NY), ("seg_0", "seg_1", "seg_2", "bin"))
    spec3 = P(SEG, None, "bin")
    return jax.shard_map(
        on_device, mesh=torus,
        in_specs=(spec3, spec3, spec3, spec3, P(SEG), P("bin")),
        out_specs=(P(SEG, "bin"), P(SEG, "bin"), P(SEG)),
        check_vma=False,
    )
```

```python
import jax
import jax.numpy as jnp
from jax import lax
from jax.experimental import pallas as pl
from jax.experimental.pallas import tpu as pltpu
from jax.sharding import Mesh
from jax.sharding import PartitionSpec as P

SEG = ("seg_0", "seg_1", "seg_2")
MESH = pl.DeviceIdType.MESH
F32 = jnp.float32
NZ, NX, NY = 8, 4, 4
LANES = 128
SEGS = 8
ROWS = 96
WROWS = 32
TILES = 64

ORDER0 = ((2, 0), (2, 1), (1, 1), (3, 0), (1, 0), (3, 1), (0, 0), (0, 1))
ORDER1 = (4, 3, 5, 2, 6, 1, 7, 0)
HALVES0 = ((4, 3, 2, 1), (5, 7, 6, 0))
INSIDE1 = (2, 1, 3, 0)
LAST = 31


def row_ids():
    return lax.broadcasted_iota(jnp.int32, (8, LANES), 0)


def spread(a, j):
    return jnp.broadcast_to(a[j : j + 1, :], (8, LANES))


def spectra_tile(tile, mr, mi, dr, di, keep, hbuf, put):
    lanes = pl.ds(pl.multiple_of(tile * LANES, LANES), LANES)
    rows = row_ids()
    total = [jnp.zeros((8, LANES), F32) for _ in range(13)]
    held = [jnp.zeros((8, LANES), F32) for _ in range(4)]
    for s in range(SEGS):
        a = mr[s, :, lanes].astype(F32)
        b = mi[s, :, lanes].astype(F32)
        hr = dr[s, :, lanes].astype(F32)
        hi = di[s, :, lanes].astype(F32)
        v = keep[s].astype(F32)
        ka, kb = a * v, b * v
        total[0] += ka * a + kb * b
        for r in range(1, 5):
            ra, rb = pltpu.roll(a, 8 - r, 0), pltpu.roll(b, 8 - r, 0)
            total[2 * r - 1] += ka * ra + kb * rb
            total[2 * r] += kb * ra - ka * rb
        for k in range(2):
            pr, pi = spread(hr, k), spread(hi, k)
            total[9 + 2 * k] += ka * pr + kb * pi
            total[10 + 2 * k] += kb * pr - ka * pi
            held[2 * k] = jnp.where(rows == s, pr, held[2 * k])
            held[2 * k + 1] = jnp.where(rows == s, pi, held[2 * k + 1])
    total[7] = jnp.where(rows < 4, total[7], total[8])
    del total[8]
    for q in range(12):
        put(q, total[q])
    for q in range(4):
        hbuf[tile, 8 * q : 8 * q + 8, :] = held[q]


def solve(spec):
    rows = row_ids()
    re, im = [None] * 8, [None] * 8
    re[0], im[0] = spec[0], jnp.zeros((8, LANES), F32)
    for r in (1, 2, 3):
        re[r], im[r] = spec[2 * r - 1], spec[2 * r]
        re[8 - r] = pltpu.roll(re[r], r, 0)
        im[8 - r] = -pltpu.roll(im[r], r, 0)
    turned = pltpu.roll(spec[7], 4, 0)
    re[4] = jnp.where(rows < 4, spec[7], turned)
    im[4] = jnp.where(rows < 4, -turned, spec[7])
    cr, ci = [], []
    for d in range(8):
        a, b = re[d], im[d]
        for c in range(1, 8):
            a = jnp.where(rows == c, re[(d - c) % 8], a)
            b = jnp.where(rows == c, im[(d - c) % 8], b)
        cr.append(jnp.where(rows == d, a + 1.0, a))
        ci.append(b)
    cr += [spec[8], spec[10]]
    ci += [spec[9], spec[11]]
    inverse = []
    for j in range(8):
        inverse.append(1.0 / spread(cr[j], j))
        fr = jnp.where(rows > j, cr[j] * inverse[j], 0.0)
        fi = jnp.where(rows > j, ci[j] * inverse[j], 0.0)
        for d in range(j + 1, 10):
            pr, pi = spread(cr[d], j), spread(ci[d], j)
            cr[d] = cr[d] - (fr * pr - fi * pi)
            ci[d] = ci[d] - (fr * pi + fi * pr)
    out = []
    for k in (8, 9):
        yr, yi = cr[k], ci[k]
        wr, wi = jnp.zeros((8, LANES), F32), jnp.zeros((8, LANES), F32)
        for d in reversed(range(8)):
            xr, xi = spread(yr, d) * inverse[d], spread(yi, d) * inverse[d]
            wr = jnp.where(rows == d, xr, wr)
            wi = jnp.where(rows == d, xi, wi)
            yr = yr - (cr[d] * xr - ci[d] * xi)
            yi = yi - (cr[d] * xi + ci[d] * xr)
        out += [wr, wi]
    return out


def row_sums(parts):
    rows = row_ids()
    low = rows < 4
    merged = []
    for s in range(4):
        a, b = parts[s], parts[s + 4]
        merged.append(jnp.where(low, a, b) + pltpu.roll(jnp.where(low, b, a), 4, 0))
    for step in (2, 1):
        first = (rows & step) == 0
        merged = [
            jnp.where(
                first,
                merged[s] + pltpu.roll(merged[s], 8 - step, 0),
                merged[s + step] + pltpu.roll(merged[s + step], step, 0),
            )
            for s in range(step)
        ]
    return merged[0]


def clean_tile(tile, mr, mi, inter, wbuf, hbuf, out_r, out_i):
    lanes = pl.ds(pl.multiple_of(tile * LANES, LANES), LANES)
    w = [wbuf[tile, 8 * q : 8 * q + 8, :] for q in range(4)]
    parts = [[], [], [], []]
    for s in range(SEGS):
        a = mr[s, :, lanes].astype(F32)
        b = mi[s, :, lanes].astype(F32)
        for k in range(2):
            parts[2 * k].append(w[2 * k] * a + w[2 * k + 1] * b)
            parts[2 * k + 1].append(w[2 * k] * b - w[2 * k + 1] * a)
    g = [hbuf[tile, 8 * q : 8 * q + 8, :] - row_sums(parts[q]) for q in range(4)]
    real = g[0] * g[2] + g[1] * g[3]
    out_r[:, lanes] = real
    out_i[:, lanes] = g[1] * g[2] - g[0] * g[3]
    return real * inter[pl.ds(tile, 1), :]


def kernel(
    mr_hbm, mi_hbm, dr_hbm, di_hbm, keep_hbm, inter_hbm, out_r, out_i, est,
    mr, mi, dr, di, keep, inter, acc, outbox, inbox, rbuf, pbuf, wbuf, hbuf, num, ybuf,
    m_in, d_in, sent, p_recv, r_recv, q_recv, z_recv, x_recv, f_recv, w_recv, y_recv,
):
    z, x, c = lax.axis_index("seg_0"), lax.axis_index("seg_1"), lax.axis_index("seg_2")
    y = lax.axis_index("bin")

    def at_z(d):
        return {"seg_0": lax.rem(z + d, NZ)}

    def at_x(d):
        return {"seg_1": lax.rem(x + d, NX)}

    def at_y(d):
        return {"bin": lax.rem(y + d, NY)}

    partner = {"seg_2": 1 - c}

    barrier = pltpu.get_barrier_semaphore()
    peers = [at_z(d) for d in (1, 2, 6, 7)] + [at_x(d) for d in range(1, NX)]
    peers += [at_y(d) for d in range(1, NY)] + [partner]
    for peer in peers:
        pl.semaphore_signal(barrier, inc=1, device_id=peer, device_id_type=MESH)

    on_core0 = c == 0

    def tile0(xo, zo):
        return lax.rem(x + xo, NX) * 8 + lax.rem(z + zo, NZ)

    def tile1(zo, xo):
        return 32 + lax.rem(z + zo, NZ) * 4 + lax.rem(x + xo, NX)

    def fetch(src, dst, first, tiles, sem):
        lanes = pl.ds(pl.multiple_of(first * LANES, 4 * LANES), tiles * LANES)
        return pltpu.make_async_copy(src.at[:, :, lanes], dst.at[:, :, lanes], sem)

    class Pair:
        def __init__(self, first, tiles, sem):
            self.parts = [fetch(mr_hbm, mr, first, tiles, sem), fetch(mi_hbm, mi, first, tiles, sem)]
            whole = mr.at[:, :, pl.ds(0, 2 * tiles * LANES)]
            self.both = pltpu.make_async_copy(whole, whole, sem)

        def start(self):
            for part in self.parts:
                part.start()

        def wait(self):
            self.both.wait()

    loads0, loads1 = {}, {}
    for at, xo in enumerate((2, 1, 3, 0)):
        loads0[xo] = Pair(lax.rem(x + xo, NX) * 8, 8, m_in.at[at])
    for at, zo in enumerate(ORDER1):
        loads1[zo] = Pair(32 + lax.rem(z + zo, NZ) * 4, 4, m_in.at[4 + at])
    small = [
        pltpu.make_async_copy(keep_hbm, keep, d_in.at[0]),
        pltpu.make_async_copy(dr_hbm, dr, d_in.at[1]),
        pltpu.make_async_copy(di_hbm, di, d_in.at[2]),
        pltpu.make_async_copy(inter_hbm, inter, d_in.at[3]),
    ]
    early = small[:3] + [loads0[2], loads1[4], loads1[3]]
    late = [loads0[1], loads1[5], loads1[2], loads0[3], loads1[6], loads1[1], loads0[0], loads1[7], loads1[0]]
    for load in early:
        load.start()

    def copy(src, dst, send, recv, where):
        return pltpu.make_async_remote_copy(
            src_ref=src, dst_ref=dst, send_sem=send, recv_sem=recv,
            device_id=where, device_id_type=MESH,
        )

    def add_into(dst, at, src, first, count):
        for i in range(count):
            for q in range(12):
                block = pl.ds(8 * q, 8)
                dst[at + i, block, :] = dst[at + i, block, :] + src[first + i, block, :]

    def pick(four, i):
        return jnp.where(i < 2, jnp.where(i == 0, *four[:2]), jnp.where(i == 2, *four[2:]))

    def make_group(g, core0, dst):
        xo, half = ORDER0[g]

        def body(i, carry):
            zo, io = pick(HALVES0[half], i), pick(INSIDE1, i)
            tile = jnp.where(core0, tile0(xo, zo), tile1(ORDER1[g], io))

            def put(q, value):
                dst[4 * g + i, 8 * q : 8 * q + 8, :] = value

            spectra_tile(tile, mr, mi, dr, di, keep, hbuf, put)
            return carry

        lax.fori_loop(0, 4, body, 0)

    to_partner = [
        copy(outbox.at[pl.ds(4 * g, 4)], inbox.at[pl.ds(4 * g, 4)],
             sent.at[0], p_recv.at[g], partner)
        for g in range(8)
    ]

    def hop(first, count, place, slot, where):
        return copy(acc.at[pl.ds(first, count)], rbuf.at[pl.ds(place, count)],
                    sent.at[1], r_recv.at[slot], where)

    zero_at = ((0, 2, 8, 10, 16, 18), (4, 6, 12, 14, 20, 22))
    zero_to = ((16, 18, 28, 30, 24, 26), (20, 22, 24, 26, 28, 30))
    zero_hops = [
        [hop(zero_at[w][m], 2, 12 * w + 2 * m, 12 * w + m, at_x((1, 3)[w])) for m in range(6)]
        for w in range(2)
    ]
    one_far = [
        hop((0, 2)[w], 2, 14 * w, 13 * w, at_z((2, 6)[w])) for w in range(2)
    ]
    inside = ((2, 3, 0, 1), (0, 1, 2, 3))
    levels = ((4, 12, 20, 28), (8, 16, 24, 28))
    one_hops = [
        [
            hop(levels[w][m // 4] + inside[w][m % 4], 1, 14 * w + 2 + m, 13 * w + 1 + m, at_z((1, 7)[w]))
            for m in range(12)
        ]
        for w in range(2)
    ]

    def combine(g):
        with jax.named_scope(f"comb{g}"):
            to_partner[g].wait_recv()
            add_into(acc, 4 * g, inbox, 4 * g, 4)

    def zero_take(m):
        for w in range(2):
            with jax.named_scope(f"zt{m}_{w}"):
                zero_hops[w][m].wait_recv()
                add_into(acc, zero_to[w][m], rbuf, 12 * w + 2 * m, 2)
                if m < 2:
                    zero_hops[w][4 + m].start()

    def far_take():
        for w in range(2):
            with jax.named_scope(f"of_{w}"):
                one_far[w].wait_recv()
                add_into(acc, (12, 18)[w], rbuf, 14 * w, 2)

    def one_take(ms):
        for m in ms:
            for w in range(2):
                with jax.named_scope(f"ot{m}_{w}"):
                    one_hops[w][m].wait_recv()
                    add_into(acc, levels[w][m // 4 + 1] + inside[w][m % 4], rbuf, 14 * w + 2 + m, 1)
                    if m < 8:
                        one_hops[w][m + 4].start()

    def zero_send(w, ms):
        for m in ms:
            zero_hops[w][m].start()

    place0 = {zo: 24 + 4 * h + i for h in range(2) for i, zo in enumerate(HALVES0[h])}

    def last_of(src, dst, slot, where):
        return copy(src, dst, sent.at[2], q_recv.at[slot], where)

    top, low = pl.ds(0, ROWS // 2), pl.ds(ROWS // 2, ROWS // 2)
    via = [
        last_of(acc.at[place0[4], top], pbuf.at[2, top], 0, at_z(2)),
        last_of(acc.at[place0[4], low], pbuf.at[2, low], 1, at_z(6)),
        last_of(acc.at[place0[3]], pbuf.at[0], 2, at_z(1)),
        last_of(acc.at[place0[5]], pbuf.at[1], 3, at_z(7)),
    ]
    zero_last = {
        d: last_of(acc.at[place0[d]], pbuf.at[3 + i], 4 + i, at_z(d)) for i, d in enumerate((1, 7, 2, 6))
    }
    one_last = {
        d: last_of(acc.at[28 + INSIDE1.index(d)], pbuf.at[d], d, at_x(d)) for d in (2, 1, 3)
    }

    def add_rows(at, slot, first, blocks):
        for q in range(blocks):
            block = pl.ds(first + 8 * q, 8)
            acc[at, block, :] = acc[at, block, :] + pbuf[slot, block, :]

    plan0 = {0: (0, (0, 1)), 1: (1, (0, 1)), 2: (0, (2, 3)), 3: (1, (2, 3))}

    def after(g):
        combine(g)

        @pl.when(on_core0)
        def _():
            if g in plan0:
                zero_send(*plan0[g])
            if g == 5:
                zero_take(0)
            if g == 6:
                zero_take(1)

        @pl.when(jnp.logical_not(on_core0))
        def _():
            if g == 0:
                one_far[0].start()
                one_far[1].start()
            if g in (1, 2):
                for m in range(4):
                    one_hops[g - 1][m].start()
            if g == 6:
                one_take((0, 1))
                far_take()
                one_take((2, 3))

    for g in range(8):
        xo, half = ORDER0[g]
        with jax.named_scope(f"load{g}"):
            if g == 0:
                for load in small[:3]:
                    load.wait()
            loads1[ORDER1[g]].wait()
            if (xo, half) in ((2, 0), (1, 1), (3, 0), (0, 0)):
                loads0[xo].wait()
        if g == 0:
            for load in late + small[3:]:
                load.start()
        with jax.named_scope(f"mk_other{g}"):
            make_group(g, jnp.logical_not(on_core0), outbox)
        if g == 0:
            with jax.named_scope("barrier"):
                pl.semaphore_wait(barrier, len(peers))
        with jax.named_scope(f"mk_own{g}"):
            to_partner[g].start()
            make_group(g, on_core0, acc)
        if g:
            after(g - 1)
    after(7)

    @pl.when(on_core0)
    def _():
        zero_take(2)
        zero_take(4)
        for step in via + [zero_last[7]]:
            step.start()
        zero_take(3)
        zero_take(5)
        zero_last[1].start()
        with jax.named_scope("p2_via"):
            via[2].wait_recv()
            add_rows(place0[2], 0, 0, 12)
            via[0].wait_recv()
            add_rows(place0[2], 2, 0, 6)
            zero_last[2].start()
            via[3].wait_recv()
            add_rows(place0[6], 1, 0, 12)
            via[1].wait_recv()
            add_rows(place0[6], 2, ROWS // 2, 6)
            zero_last[6].start()
        for i, d in enumerate((1, 7, 2, 6)):
            with jax.named_scope(f"p2_{d}"):
                zero_last[d].wait_recv()
                add_rows(LAST, 3 + i, 0, 12)

    @pl.when(jnp.logical_not(on_core0))
    def _():
        one_take(range(4, 11))
        one_last[2].start()
        one_last[3].start()
        one_take((11,))
        one_last[1].start()
        for d in (2, 3, 1):
            with jax.named_scope(f"q2_{d}"):
                one_last[d].wait_recv()
                add_rows(LAST, d, 0, 12)

    with jax.named_scope("solve"):
        spec = [acc[LAST, 8 * q : 8 * q + 8, :] for q in range(12)]
        filters = solve(spec)

    def tile_of(core, zz, xx):
        return jnp.where(core == 0, xx * 8 + zz, 32 + zz * 4 + xx)

    mine = tile_of(c, z, x)
    for q in range(4):
        wbuf[mine, 8 * q : 8 * q + 8, :] = filters[q]

    def w_copy(tile, recv, where):
        return copy(wbuf.at[tile], wbuf.at[tile], sent.at[3], recv, where)

    far_first = (4, 3, 5, 2, 6, 1, 7)
    along_z = {d: w_copy(mine, z_recv.at[d - 1], at_z(d)) for d in far_first}
    for d in far_first:
        along_z[d].start()

    small[3].wait()
    square = inter[0:8, :] * inter[0:8, :]
    for i in range(1, 8):
        square = square + inter[8 * i : 8 * i + 8, :] * inter[8 * i : 8 * i + 8, :]
    num[...] = jnp.zeros_like(num)

    def tile_from(core, dz, dx):
        return tile_of(core, lax.rem(z + NZ - dz, NZ), lax.rem(x + NX - dx, NX))

    def got(tile, sem, where):
        w_copy(tile, sem, where).wait_recv()

    def cleaned(tile):
        num[...] += clean_tile(tile, mr, mi, inter, wbuf, hbuf, out_r, out_i)

    near_first = (0, 1, 7, 2, 6, 3, 5, 4)

    blocks = [[(d, 0) for d in near_first[:4]], [(d, 0) for d in near_first[4:]]]
    blocks += [[(d, dx) for d in near_first[4 * i : 4 * i + 4] for dx in (1, 3)] for i in range(2)]
    blocks += [[(d, 2) for d in near_first[2 * i : 2 * i + 2]] for i in range(4)]
    block_of = {item: i for i, block in enumerate(blocks) for item in block}

    def share(d, dx, tile):
        w_copy(tile, w_recv.at[block_of[d, dx]], partner).start()

    def got_block(i):
        with jax.named_scope(f"gp{i}"):
            whole = wbuf.at[pl.ds(0, len(blocks[i]))]
            copy(whole, whole, sent.at[3], w_recv.at[i], partner).wait_recv()

    def clean_block(i, first=0, last=8):
        for d, dx in blocks[i][first:last]:
            cleaned(tile_from(1 - c, d, dx))

    for d in near_first:
        tile = tile_from(c, d, 0)
        if d:
            with jax.named_scope(f"gz{d}"):
                got(tile, z_recv.at[d - 1], at_z(NZ - d))
        for way, dx in ((0, 1), (1, 3)):
            w_copy(tile, x_recv.at[way, d], at_x(dx)).start()
        share(d, 0, tile)
        cleaned(tile)
    for i, d in enumerate(near_first):
        for way, dx in ((0, 1), (1, 3)):
            tile = tile_from(c, d, dx)
            with jax.named_scope(f"gx{d}_{dx}"):
                got(tile, x_recv.at[way, d], at_x(NX - dx))
            if way == i % 2:
                w_copy(tile, f_recv.at[d], at_x(dx)).start()
            share(d, dx, tile)
            cleaned(tile)
    for i, d in enumerate(near_first):
        if i in (0, 1):
            got_block(i)
            clean_block(i)
        if i in (2, 4):
            got_block(i // 2 + 1)
            clean_block(i // 2 + 1, 0, 4)
        if i in (3, 5):
            clean_block(i // 2 + 1, 4, 8)
        tile = tile_from(c, d, 2)
        with jax.named_scope(f"gf{d}"):
            got(tile, f_recv.at[d], at_x(1 if i % 2 == 1 else 3))
        share(d, 2, tile)
        cleaned(tile)
    for i in range(4, 8):
        got_block(i)
        clean_block(i)

    with jax.named_scope("ysum"):
        ybuf[y, 0:8, :] = num[...]
        ybuf[y, 8:16, :] = square
        over_y = [
            copy(ybuf.at[y], ybuf.at[y], sent.at[4], y_recv.at[d - 1], at_y(d)) for d in range(1, NY)
        ]
        for step in over_y:
            step.start()
        for d in range(1, NY):
            src = lax.rem(y + NY - d, NY)
            copy(ybuf.at[src], ybuf.at[src], sent.at[4], y_recv.at[d - 1], at_y(NY - d)).wait_recv()
    top, norm = ybuf[0, 0:8, :], ybuf[0, 8:16, :]
    for i in range(1, NY):
        top, norm = top + ybuf[i, 0:8, :], norm + ybuf[i, 8:16, :]
    top = jnp.sum(top, axis=1, keepdims=True)
    norm = jnp.sum(jnp.sum(norm, axis=1, keepdims=True), axis=0, keepdims=True)
    value = jnp.broadcast_to(top / jnp.sqrt(norm), (8, LANES))
    diagonal = row_ids() == lax.broadcasted_iota(jnp.int32, (8, LANES), 1)
    est[...] = jnp.sum(jnp.where(diagonal, value, 0.0), axis=0, keepdims=True)

    def left(ref, sem):
        copy(ref, ref, sem, z_recv.at[0], partner).wait_send()

    left(acc, sent.at[0])
    left(wbuf.at[pl.ds(0, 63)], sent.at[3])
    left(ybuf.at[pl.ds(0, NY - 1)], sent.at[4])

    @pl.when(on_core0)
    def _():
        left(acc.at[pl.ds(0, 24)], sent.at[1])
        left(acc.at[pl.ds(0, 7)], sent.at[2])

    @pl.when(jnp.logical_not(on_core0))
    def _():
        left(acc.at[pl.ds(0, 28)], sent.at[1])
        left(acc.at[pl.ds(0, 3)], sent.at[2])


def on_device(magnet_real, magnet_imag, detector_real, detector_imag, valid, intersection):
    bins = magnet_real.shape[2]
    assert bins == TILES * LANES and magnet_real.shape[:2] == (SEGS, 8)
    dma = pltpu.SemaphoreType.DMA
    vmem = pl.BlockSpec(memory_space=pltpu.VMEM)
    hbm = pl.BlockSpec(memory_space=pl.ANY)
    cleaned_real, cleaned_imag, estimate = pl.pallas_call(
        kernel,
        out_shape=(
            pltpu.VMEM((SEGS, bins), F32),
            pltpu.VMEM((SEGS, bins), F32),
            pltpu.VMEM((1, LANES), F32),
        ),
        in_specs=[hbm] * 6,
        out_specs=(vmem, vmem, vmem),
        scratch_shapes=[
            pltpu.VMEM(magnet_real.shape, magnet_real.dtype),
            pltpu.VMEM(magnet_imag.shape, magnet_imag.dtype),
            pltpu.VMEM(detector_real.shape, detector_real.dtype),
            pltpu.VMEM(detector_imag.shape, detector_imag.dtype),
            pltpu.SMEM((SEGS,), jnp.int32),
            pltpu.VMEM((TILES, LANES), F32),
            pltpu.VMEM((32, ROWS, LANES), F32),
            pltpu.VMEM((32, ROWS, LANES), F32),
            pltpu.VMEM((32, ROWS, LANES), F32),
            pltpu.VMEM((28, ROWS, LANES), F32),
            pltpu.VMEM((8, ROWS, LANES), F32),
            pltpu.VMEM((TILES, WROWS, LANES), F32),
            pltpu.VMEM((TILES, 32, LANES), F32),
            pltpu.VMEM((8, LANES), F32),
            pltpu.VMEM((NY, 16, LANES), F32),
            dma((12,)), dma((4,)), dma((5,)), dma((8,)), dma((26,)), dma((8,)), dma((7,)),
            dma((2, 8)), dma((8,)), dma((8,)), dma((3,)),
        ],
        compiler_params=pltpu.CompilerParams(collective_id=0, has_side_effects=True),
    )(
        magnet_real, magnet_imag, detector_real, detector_imag,
        valid, intersection.reshape(TILES, LANES),
    )
    return cleaned_real, cleaned_imag, estimate[0, :SEGS]


def solution(mesh):
    assert mesh.shape["seg"] == NZ * NX * 2 and mesh.shape["bin"] == NY
    torus = Mesh(mesh.devices.reshape(NZ, NX, 2, NY), ("seg_0", "seg_1", "seg_2", "bin"))
    spec3 = P(SEG, None, "bin")
    return jax.shard_map(
        on_device, mesh=torus,
        in_specs=(spec3, spec3, spec3, spec3, P(SEG), P("bin")),
        out_specs=(P(SEG, "bin"), P(SEG, "bin"), P(SEG)),
        check_vma=False,
    )
```

```python
import jax
import jax.numpy as jnp
from jax import lax
from jax.experimental import pallas as pl
from jax.experimental.pallas import tpu as pltpu
from jax.sharding import Mesh
from jax.sharding import PartitionSpec as P

SEG = ("seg_0", "seg_1", "seg_2")
MESH = pl.DeviceIdType.MESH
F32 = jnp.float32
NZ, NX, NY = 8, 4, 4
LANES = 128
SEGS = 8
ROWS = 96
WROWS = 32
TILES = 64

ORDER0 = ((2, 0), (2, 1), (1, 1), (3, 0), (1, 0), (3, 1), (0, 0), (0, 1))
ORDER1 = (4, 3, 5, 2, 6, 1, 7, 0)
HALVES0 = ((4, 3, 2, 1), (5, 7, 6, 0))
INSIDE1 = (2, 1, 3, 0)
LAST = 31


def row_ids():
    return lax.broadcasted_iota(jnp.int32, (8, LANES), 0)


def spread(a, j):
    return jnp.broadcast_to(a[j : j + 1, :], (8, LANES))


def spectra_tile(tile, mr, mi, dr, di, keep, hbuf, put):
    lanes = pl.ds(pl.multiple_of(tile * LANES, LANES), LANES)
    rows = row_ids()
    total = [jnp.zeros((8, LANES), F32) for _ in range(13)]
    held = [jnp.zeros((8, LANES), F32) for _ in range(4)]
    for s in range(SEGS):
        a = mr[s, :, lanes].astype(F32)
        b = mi[s, :, lanes].astype(F32)
        hr = dr[s, :, lanes].astype(F32)
        hi = di[s, :, lanes].astype(F32)
        v = keep[s].astype(F32)
        ka, kb = a * v, b * v
        total[0] += ka * a + kb * b
        for r in range(1, 5):
            ra, rb = pltpu.roll(a, 8 - r, 0), pltpu.roll(b, 8 - r, 0)
            total[2 * r - 1] += ka * ra + kb * rb
            total[2 * r] += kb * ra - ka * rb
        for k in range(2):
            pr, pi = spread(hr, k), spread(hi, k)
            total[9 + 2 * k] += ka * pr + kb * pi
            total[10 + 2 * k] += kb * pr - ka * pi
            held[2 * k] = jnp.where(rows == s, pr, held[2 * k])
            held[2 * k + 1] = jnp.where(rows == s, pi, held[2 * k + 1])
    total[7] = jnp.where(rows < 4, total[7], total[8])
    del total[8]
    for q in range(12):
        put(q, total[q])
    for q in range(4):
        hbuf[tile, 8 * q : 8 * q + 8, :] = held[q]


def solve(spec):
    rows = row_ids()
    re, im = [None] * 8, [None] * 8
    re[0], im[0] = spec[0], jnp.zeros((8, LANES), F32)
    for r in (1, 2, 3):
        re[r], im[r] = spec[2 * r - 1], spec[2 * r]
        re[8 - r] = pltpu.roll(re[r], r, 0)
        im[8 - r] = -pltpu.roll(im[r], r, 0)
    turned = pltpu.roll(spec[7], 4, 0)
    re[4] = jnp.where(rows < 4, spec[7], turned)
    im[4] = jnp.where(rows < 4, -turned, spec[7])
    cr, ci = [], []
    for d in range(8):
        a, b = re[d], im[d]
        for c in range(1, 8):
            a = jnp.where(rows == c, re[(d - c) % 8], a)
            b = jnp.where(rows == c, im[(d - c) % 8], b)
        cr.append(jnp.where(rows == d, a + 1.0, a))
        ci.append(b)
    cr += [spec[8], spec[10]]
    ci += [spec[9], spec[11]]
    inverse = []
    for j in range(8):
        inverse.append(1.0 / spread(cr[j], j))
        fr = jnp.where(rows > j, cr[j] * inverse[j], 0.0)
        fi = jnp.where(rows > j, ci[j] * inverse[j], 0.0)
        for d in range(j + 1, 10):
            pr, pi = spread(cr[d], j), spread(ci[d], j)
            cr[d] = cr[d] - (fr * pr - fi * pi)
            ci[d] = ci[d] - (fr * pi + fi * pr)
    out = []
    for k in (8, 9):
        yr, yi = cr[k], ci[k]
        wr, wi = jnp.zeros((8, LANES), F32), jnp.zeros((8, LANES), F32)
        for d in reversed(range(8)):
            xr, xi = spread(yr, d) * inverse[d], spread(yi, d) * inverse[d]
            wr = jnp.where(rows == d, xr, wr)
            wi = jnp.where(rows == d, xi, wi)
            yr = yr - (cr[d] * xr - ci[d] * xi)
            yi = yi - (cr[d] * xi + ci[d] * xr)
        out += [wr, wi]
    return out


def row_sums(parts):
    rows = row_ids()
    low = rows < 4
    merged = []
    for s in range(4):
        a, b = parts[s], parts[s + 4]
        merged.append(jnp.where(low, a, b) + pltpu.roll(jnp.where(low, b, a), 4, 0))
    for step in (2, 1):
        first = (rows & step) == 0
        merged = [
            jnp.where(
                first,
                merged[s] + pltpu.roll(merged[s], 8 - step, 0),
                merged[s + step] + pltpu.roll(merged[s + step], step, 0),
            )
            for s in range(step)
        ]
    return merged[0]


def clean_tile(tile, mr, mi, inter, wbuf, hbuf, out_r, out_i):
    lanes = pl.ds(pl.multiple_of(tile * LANES, LANES), LANES)
    w = [wbuf[tile, 8 * q : 8 * q + 8, :] for q in range(4)]
    parts = [[], [], [], []]
    for s in range(SEGS):
        a = mr[s, :, lanes].astype(F32)
        b = mi[s, :, lanes].astype(F32)
        for k in range(2):
            parts[2 * k].append(w[2 * k] * a + w[2 * k + 1] * b)
            parts[2 * k + 1].append(w[2 * k] * b - w[2 * k + 1] * a)
    g = [hbuf[tile, 8 * q : 8 * q + 8, :] - row_sums(parts[q]) for q in range(4)]
    real = g[0] * g[2] + g[1] * g[3]
    out_r[:, lanes] = real
    out_i[:, lanes] = g[1] * g[2] - g[0] * g[3]
    return real * inter[pl.ds(tile, 1), :]


def kernel(
    mr_hbm, mi_hbm, dr_hbm, di_hbm, keep_hbm, inter_hbm, out_r, out_i, est,
    mr, mi, dr, di, keep, inter, acc, outbox, inbox, rbuf, pbuf, wbuf, hbuf, num, ybuf,
    m_in, d_in, sent, p_recv, r_recv, q_recv, z_recv, x_recv, w_recv, y_recv,
):
    z, x, c = lax.axis_index("seg_0"), lax.axis_index("seg_1"), lax.axis_index("seg_2")
    y = lax.axis_index("bin")

    def at_z(d):
        return {"seg_0": lax.rem(z + d, NZ)}

    def at_x(d):
        return {"seg_1": lax.rem(x + d, NX)}

    def at_y(d):
        return {"bin": lax.rem(y + d, NY)}

    partner = {"seg_2": 1 - c}

    barrier = pltpu.get_barrier_semaphore()
    peers = [at_z(d) for d in (1, 2, 6, 7)] + [at_x(d) for d in range(1, NX)]
    peers += [at_y(d) for d in range(1, NY)] + [partner]
    for peer in peers:
        pl.semaphore_signal(barrier, inc=1, device_id=peer, device_id_type=MESH)

    on_core0 = c == 0

    def tile0(xo, zo):
        return lax.rem(x + xo, NX) * 8 + lax.rem(z + zo, NZ)

    def tile1(zo, xo):
        return 32 + lax.rem(z + zo, NZ) * 4 + lax.rem(x + xo, NX)

    def fetch(src, dst, first, tiles, sem):
        lanes = pl.ds(pl.multiple_of(first * LANES, 4 * LANES), tiles * LANES)
        return pltpu.make_async_copy(src.at[:, :, lanes], dst.at[:, :, lanes], sem)

    class Pair:
        def __init__(self, first, tiles, sem):
            self.parts = [fetch(mr_hbm, mr, first, tiles, sem), fetch(mi_hbm, mi, first, tiles, sem)]
            whole = mr.at[:, :, pl.ds(0, 2 * tiles * LANES)]
            self.both = pltpu.make_async_copy(whole, whole, sem)

        def start(self):
            for part in self.parts:
                part.start()

        def wait(self):
            self.both.wait()

    loads0, loads1 = {}, {}
    for at, xo in enumerate((2, 1, 3, 0)):
        loads0[xo] = Pair(lax.rem(x + xo, NX) * 8, 8, m_in.at[at])
    for at, zo in enumerate(ORDER1):
        loads1[zo] = Pair(32 + lax.rem(z + zo, NZ) * 4, 4, m_in.at[4 + at])
    small = [
        pltpu.make_async_copy(keep_hbm, keep, d_in.at[0]),
        pltpu.make_async_copy(dr_hbm, dr, d_in.at[1]),
        pltpu.make_async_copy(di_hbm, di, d_in.at[2]),
        pltpu.make_async_copy(inter_hbm, inter, d_in.at[3]),
    ]
    early = small[:3] + [loads0[2], loads1[4], loads1[3]]
    late = [loads0[1], loads1[5], loads1[2], loads0[3], loads1[6], loads1[1], loads0[0], loads1[7], loads1[0]]
    for load in early:
        load.start()

    def copy(src, dst, send, recv, where):
        return pltpu.make_async_remote_copy(
            src_ref=src, dst_ref=dst, send_sem=send, recv_sem=recv,
            device_id=where, device_id_type=MESH,
        )

    def add_into(dst, at, src, first, count):
        for i in range(count):
            for q in range(12):
                block = pl.ds(8 * q, 8)
                dst[at + i, block, :] = dst[at + i, block, :] + src[first + i, block, :]

    def pick(four, i):
        return jnp.where(i < 2, jnp.where(i == 0, *four[:2]), jnp.where(i == 2, *four[2:]))

    def make_group(g, core0, dst):
        xo, half = ORDER0[g]

        def body(i, carry):
            zo, io = pick(HALVES0[half], i), pick(INSIDE1, i)
            tile = jnp.where(core0, tile0(xo, zo), tile1(ORDER1[g], io))

            def put(q, value):
                dst[4 * g + i, 8 * q : 8 * q + 8, :] = value

            spectra_tile(tile, mr, mi, dr, di, keep, hbuf, put)
            return carry

        lax.fori_loop(0, 4, body, 0)

    to_partner = [
        copy(outbox.at[pl.ds(4 * g, 4)], inbox.at[pl.ds(4 * g, 4)],
             sent.at[0], p_recv.at[g], partner)
        for g in range(8)
    ]

    def hop(first, count, place, slot, where):
        return copy(acc.at[pl.ds(first, count)], rbuf.at[pl.ds(place, count)],
                    sent.at[1], r_recv.at[slot], where)

    zero_at = ((0, 2, 8, 10, 16, 18), (4, 6, 12, 14, 20, 22))
    zero_to = ((16, 18, 28, 30, 24, 26), (20, 22, 24, 26, 28, 30))
    zero_hops = [
        [hop(zero_at[w][m], 2, 12 * w + 2 * m, 12 * w + m, at_x((1, 3)[w])) for m in range(6)]
        for w in range(2)
    ]
    one_far = [
        hop((0, 2)[w], 2, 14 * w, 13 * w, at_z((2, 6)[w])) for w in range(2)
    ]
    inside = ((2, 3, 0, 1), (0, 1, 2, 3))
    levels = ((4, 12, 20, 28), (8, 16, 24, 28))
    one_hops = [
        [
            hop(levels[w][m // 4] + inside[w][m % 4], 1, 14 * w + 2 + m, 13 * w + 1 + m, at_z((1, 7)[w]))
            for m in range(12)
        ]
        for w in range(2)
    ]

    def combine(g):
        with jax.named_scope(f"comb{g}"):
            to_partner[g].wait_recv()
            add_into(acc, 4 * g, inbox, 4 * g, 4)

    def zero_take(m):
        for w in range(2):
            with jax.named_scope(f"zt{m}_{w}"):
                zero_hops[w][m].wait_recv()
                add_into(acc, zero_to[w][m], rbuf, 12 * w + 2 * m, 2)
                if m < 2:
                    zero_hops[w][4 + m].start()

    def far_take():
        for w in range(2):
            with jax.named_scope(f"of_{w}"):
                one_far[w].wait_recv()
                add_into(acc, (12, 18)[w], rbuf, 14 * w, 2)

    def one_take(ms):
        for m in ms:
            for w in range(2):
                with jax.named_scope(f"ot{m}_{w}"):
                    one_hops[w][m].wait_recv()
                    add_into(acc, levels[w][m // 4 + 1] + inside[w][m % 4], rbuf, 14 * w + 2 + m, 1)
                    if m < 8:
                        one_hops[w][m + 4].start()

    def zero_send(w, ms):
        for m in ms:
            zero_hops[w][m].start()

    place0 = {zo: 24 + 4 * h + i for h in range(2) for i, zo in enumerate(HALVES0[h])}

    def last_of(src, dst, slot, where):
        return copy(src, dst, sent.at[2], q_recv.at[slot], where)

    top, low = pl.ds(0, ROWS // 2), pl.ds(ROWS // 2, ROWS // 2)
    via = [
        last_of(acc.at[place0[4], top], pbuf.at[2, top], 0, at_z(2)),
        last_of(acc.at[place0[4], low], pbuf.at[2, low], 1, at_z(6)),
        last_of(acc.at[place0[3]], pbuf.at[0], 2, at_z(1)),
        last_of(acc.at[place0[5]], pbuf.at[1], 3, at_z(7)),
    ]
    zero_last = {
        d: last_of(acc.at[place0[d]], pbuf.at[3 + i], 4 + i, at_z(d)) for i, d in enumerate((1, 7, 2, 6))
    }
    one_last = {
        d: last_of(acc.at[28 + INSIDE1.index(d)], pbuf.at[d], d, at_x(d)) for d in (2, 1, 3)
    }

    def add_rows(at, slot, first, blocks):
        for q in range(blocks):
            block = pl.ds(first + 8 * q, 8)
            acc[at, block, :] = acc[at, block, :] + pbuf[slot, block, :]

    plan0 = {0: (0, (0, 1)), 1: (1, (0, 1)), 2: (0, (2, 3)), 3: (1, (2, 3))}

    def after(g):
        combine(g)

        @pl.when(on_core0)
        def _():
            if g in plan0:
                zero_send(*plan0[g])
            if g == 5:
                zero_take(0)
            if g == 6:
                zero_take(1)

        @pl.when(jnp.logical_not(on_core0))
        def _():
            if g == 0:
                one_far[0].start()
                one_far[1].start()
            if g in (1, 2):
                for m in range(4):
                    one_hops[g - 1][m].start()
            if g == 6:
                one_take((0, 1))
                far_take()
                one_take((2, 3))

    def load_group(g):
        with jax.named_scope(f"load{g}"):
            loads1[ORDER1[g]].wait()
            if ORDER0[g] in ((2, 0), (1, 1), (3, 0), (0, 0)):
                loads0[ORDER0[g][0]].wait()

    def make_other(g):
        with jax.named_scope(f"mk_other{g}"):
            make_group(g, jnp.logical_not(on_core0), outbox)

    def make_own(g):
        with jax.named_scope(f"mk_own{g}"):
            make_group(g, on_core0, acc)

    for load in small[:3]:
        load.wait()
    load_group(0)
    for load in late + small[3:]:
        load.start()
    make_other(0)
    load_group(1)
    make_other(1)
    with jax.named_scope("barrier"):
        pl.semaphore_wait(barrier, len(peers))
    to_partner[0].start()
    to_partner[1].start()
    make_own(0)
    make_own(1)
    for g in range(2, 8):
        load_group(g)
        make_other(g)
        to_partner[g].start()
        if g == 2:
            after(0)
            after(1)
        make_own(g)
        if g > 2:
            after(g - 1)
    after(7)

    @pl.when(on_core0)
    def _():
        zero_take(2)
        zero_take(4)
        for step in via + [zero_last[7]]:
            step.start()
        zero_take(3)
        zero_take(5)
        zero_last[1].start()
        with jax.named_scope("p2_via"):
            via[2].wait_recv()
            add_rows(place0[2], 0, 0, 12)
            via[0].wait_recv()
            add_rows(place0[2], 2, 0, 6)
            zero_last[2].start()
            via[3].wait_recv()
            add_rows(place0[6], 1, 0, 12)
            via[1].wait_recv()
            add_rows(place0[6], 2, ROWS // 2, 6)
            zero_last[6].start()
        for i, d in enumerate((1, 7, 2, 6)):
            with jax.named_scope(f"p2_{d}"):
                zero_last[d].wait_recv()
                add_rows(LAST, 3 + i, 0, 12)

    @pl.when(jnp.logical_not(on_core0))
    def _():
        one_take(range(4, 11))
        one_last[2].start()
        one_last[3].start()
        one_take((11,))
        one_last[1].start()
        for d in (2, 3, 1):
            with jax.named_scope(f"q2_{d}"):
                one_last[d].wait_recv()
                add_rows(LAST, d, 0, 12)

    with jax.named_scope("solve"):
        spec = [acc[LAST, 8 * q : 8 * q + 8, :] for q in range(12)]
        filters = solve(spec)

    def tile_of(core, zz, xx):
        return jnp.where(core == 0, xx * 8 + zz, 32 + zz * 4 + xx)

    mine = tile_of(c, z, x)
    for q in range(4):
        wbuf[mine, 8 * q : 8 * q + 8, :] = filters[q]

    def w_copy(tile, recv, where, count=1):
        block = wbuf.at[pl.ds(tile, count)]
        return copy(block, block, sent.at[3], recv, where)

    far_first = (4, 3, 5, 2, 6, 1, 7)

    @pl.when(on_core0)
    def _():
        for d in far_first:
            w_copy(mine, z_recv.at[d - 1], at_z(d)).start()

    @pl.when(jnp.logical_not(on_core0))
    def _():
        for d in (2, 1, 3):
            w_copy(mine, x_recv.at[d - 1, 0], at_x(d)).start()

    small[3].wait()
    square = inter[0:8, :] * inter[0:8, :]
    for i in range(1, 8):
        square = square + inter[8 * i : 8 * i + 8, :] * inter[8 * i : 8 * i + 8, :]
    num[...] = jnp.zeros_like(num)

    def tile_from(core, dz, dx):
        return tile_of(core, lax.rem(z + NZ - dz, NZ), lax.rem(x + NX - dx, NX))

    def row_from(dz):
        return 32 + 4 * lax.rem(z + NZ - dz, NZ)

    def got(name, tile, sem, where, count=1):
        with jax.named_scope(name):
            w_copy(tile, sem, where, count).wait_recv()

    def cleaned(tile):
        num[...] += clean_tile(tile, mr, mi, inter, wbuf, hbuf, out_r, out_i)

    def cleaned_row(dz):
        def body(i, carry):
            cleaned(row_from(dz) + i)
            return carry

        lax.fori_loop(0, 4, body, 0)

    near_first = (0, 1, 7, 2, 6, 3, 5, 4)

    blocks = [[(d, 0) for d in near_first[:4]], [(d, 0) for d in near_first[4:]]]
    blocks += [[(d, dx) for d in near_first[4 * i : 4 * i + 4] for dx in (1, 3)] for i in range(2)]
    blocks += [[(d, 2) for d in near_first[2 * i : 2 * i + 2]] for i in range(4)]
    block_of = {item: i for i, block in enumerate(blocks) for item in block}

    def share(d, dx, tile):
        w_copy(tile, w_recv.at[block_of[d, dx]], partner).start()

    def take_block(i):
        got(f"gp{i}", 0, w_recv.at[i], partner, len(blocks[i]))
        for d, dx in blocks[i]:
            cleaned(tile_from(0, d, dx))

    def share_row(dz):
        w_copy(row_from(dz), w_recv.at[dz], partner, 4).start()

    def take_row(dz):
        got(f"gr{dz}", row_from(dz), w_recv.at[dz], partner, 4)
        cleaned_row(dz)

    @pl.when(on_core0)
    def _():
        for d in near_first:
            tile = tile_from(0, d, 0)
            if d:
                got(f"gz{d}", tile, z_recv.at[d - 1], at_z(NZ - d))
            for dx in (2, 1, 3):
                w_copy(tile, x_recv.at[dx - 1, d], at_x(dx)).start()
            share(d, 0, tile)
            cleaned(tile)
        take_row(0)
        for i, d in enumerate(near_first):
            for dx in (1, 3):
                tile = tile_from(0, d, dx)
                got(f"gx{d}_{dx}", tile, x_recv.at[dx - 1, d], at_x(NX - dx))
                share(d, dx, tile)
                cleaned(tile)
        for i, d in enumerate(near_first):
            tile = tile_from(0, d, 2)
            got(f"gf{d}", tile, x_recv.at[1, d], at_x(2))
            share(d, 2, tile)
            cleaned(tile)
            if i in (1, 3, 5, 7):
                take_row((1, 7, 2, 6)[i // 2])
        for d in (3, 5, 4):
            take_row(d)

    @pl.when(jnp.logical_not(on_core0))
    def _():
        cleaned(mine)
        for dx in (1, 3, 2):
            got(f"rx{dx}", tile_from(1, 0, dx), x_recv.at[dx - 1, 0], at_x(NX - dx))
        for d in (2, 6, 1, 7):
            w_copy(row_from(0), z_recv.at[d - 1], at_z(d), 4).start()
        share_row(0)
        for dx in (1, 3, 2):
            cleaned(tile_from(1, 0, dx))
        for d, onward, half in ((2, 1, 0), (6, 7, 2)):
            got(f"rz{d}", row_from(d), z_recv.at[d - 1], at_z(NZ - d), 4)
            w_copy(row_from(d) + half, z_recv.at[3 if half == 0 else 7], at_z(d), 2).start()
            w_copy(row_from(d), z_recv.at[2 if half == 0 else 4], at_z(onward), 4).start()
            share_row(d)
        for d in (1, 7):
            got(f"rz{d}", row_from(d), z_recv.at[d - 1], at_z(NZ - d), 4)
            share_row(d)
        take_block(0)
        for d in (1, 7, 2, 6):
            cleaned_row(d)
        take_block(1)
        take_block(2)
        take_block(3)
        for d, back in ((3, 7), (5, 1)):
            got(f"rz{d}", row_from(d), z_recv.at[d - 1], at_z(back), 4)
            share_row(d)
            cleaned_row(d)
        got("rz4a", row_from(4), z_recv.at[3], at_z(6), 2)
        got("rz4b", row_from(4) + 2, z_recv.at[7], at_z(2), 2)
        share_row(4)
        cleaned_row(4)
        for i in range(4, 8):
            take_block(i)

    with jax.named_scope("ysum"):
        ybuf[y, 0:8, :] = num[...]
        ybuf[y, 8:16, :] = square
        over_y = [
            copy(ybuf.at[y], ybuf.at[y], sent.at[4], y_recv.at[d - 1], at_y(d)) for d in range(1, NY)
        ]
        for step in over_y:
            step.start()
        for d in range(1, NY):
            src = lax.rem(y + NY - d, NY)
            copy(ybuf.at[src], ybuf.at[src], sent.at[4], y_recv.at[d - 1], at_y(NY - d)).wait_recv()
    top, norm = ybuf[0, 0:8, :], ybuf[0, 8:16, :]
    for i in range(1, NY):
        top, norm = top + ybuf[i, 0:8, :], norm + ybuf[i, 8:16, :]
    top = jnp.sum(top, axis=1, keepdims=True)
    norm = jnp.sum(jnp.sum(norm, axis=1, keepdims=True), axis=0, keepdims=True)
    value = jnp.broadcast_to(top / jnp.sqrt(norm), (8, LANES))
    diagonal = row_ids() == lax.broadcasted_iota(jnp.int32, (8, LANES), 1)
    est[...] = jnp.sum(jnp.where(diagonal, value, 0.0), axis=0, keepdims=True)

    def left(ref, sem):
        copy(ref, ref, sem, z_recv.at[0], partner).wait_send()

    left(acc, sent.at[0])
    left(wbuf.at[pl.ds(0, 63)], sent.at[3])
    left(ybuf.at[pl.ds(0, NY - 1)], sent.at[4])

    @pl.when(on_core0)
    def _():
        left(acc.at[pl.ds(0, 24)], sent.at[1])
        left(acc.at[pl.ds(0, 7)], sent.at[2])

    @pl.when(jnp.logical_not(on_core0))
    def _():
        left(acc.at[pl.ds(0, 28)], sent.at[1])
        left(acc.at[pl.ds(0, 3)], sent.at[2])


def on_device(magnet_real, magnet_imag, detector_real, detector_imag, valid, intersection):
    bins = magnet_real.shape[2]
    assert bins == TILES * LANES and magnet_real.shape[:2] == (SEGS, 8)
    dma = pltpu.SemaphoreType.DMA
    vmem = pl.BlockSpec(memory_space=pltpu.VMEM)
    hbm = pl.BlockSpec(memory_space=pl.ANY)
    cleaned_real, cleaned_imag, estimate = pl.pallas_call(
        kernel,
        out_shape=(
            pltpu.VMEM((SEGS, bins), F32),
            pltpu.VMEM((SEGS, bins), F32),
            pltpu.VMEM((1, LANES), F32),
        ),
        in_specs=[hbm] * 6,
        out_specs=(vmem, vmem, vmem),
        scratch_shapes=[
            pltpu.VMEM(magnet_real.shape, magnet_real.dtype),
            pltpu.VMEM(magnet_imag.shape, magnet_imag.dtype),
            pltpu.VMEM(detector_real.shape, detector_real.dtype),
            pltpu.VMEM(detector_imag.shape, detector_imag.dtype),
            pltpu.SMEM((SEGS,), jnp.int32),
            pltpu.VMEM((TILES, LANES), F32),
            pltpu.VMEM((32, ROWS, LANES), F32),
            pltpu.VMEM((32, ROWS, LANES), F32),
            pltpu.VMEM((32, ROWS, LANES), F32),
            pltpu.VMEM((28, ROWS, LANES), F32),
            pltpu.VMEM((8, ROWS, LANES), F32),
            pltpu.VMEM((TILES, WROWS, LANES), F32),
            pltpu.VMEM((TILES, 32, LANES), F32),
            pltpu.VMEM((8, LANES), F32),
            pltpu.VMEM((NY, 16, LANES), F32),
            dma((12,)), dma((4,)), dma((5,)), dma((8,)), dma((26,)), dma((8,)), dma((8,)),
            dma((3, 8)), dma((8,)), dma((3,)),
        ],
        compiler_params=pltpu.CompilerParams(collective_id=0, has_side_effects=True),
    )(
        magnet_real, magnet_imag, detector_real, detector_imag,
        valid, intersection.reshape(TILES, LANES),
    )
    return cleaned_real, cleaned_imag, estimate[0, :SEGS]


def solution(mesh):
    assert mesh.shape["seg"] == NZ * NX * 2 and mesh.shape["bin"] == NY
    torus = Mesh(mesh.devices.reshape(NZ, NX, 2, NY), ("seg_0", "seg_1", "seg_2", "bin"))
    spec3 = P(SEG, None, "bin")
    return jax.shard_map(
        on_device, mesh=torus,
        in_specs=(spec3, spec3, spec3, spec3, P(SEG), P("bin")),
        out_specs=(P(SEG, "bin"), P(SEG, "bin"), P(SEG)),
        check_vma=False,
    )
```
